32 devices in a mesh: replica: 1 (over z), heads: 4 (over y), model: 8 (over x, core).
Axes of the slice: x: 4, y: 4, z: 1, core: 2. Of those that a mesh axis runs over, the one named last changes fastest.
The devices are a block of a 4x4x8 slice.
Arguments:
- tokens: bfloat16 [256, 4096], P('replica')
- w_query: bfloat16 [4096, 4096], P(None, ('heads', 'model'))
- w_key: bfloat16 [4096, 1024], replicated
- w_value: bfloat16 [4096, 1024], replicated
- w_out: bfloat16 [4096, 4096], P(('heads', 'model'))
- key_cache: bfloat16 [256, 8, 1024, 128], P(('replica', 'model'))
- value_cache: bfloat16 [256, 8, 1024, 128], P(('replica', 'model'))
- lengths: int32 [256], P(('replica', 'model'))
Outputs:
- output 1: bfloat16 [256, 4096], P('replica')
- output 2: bfloat16 [256, 8, 128], P(('replica', 'model'))
- output 3: bfloat16 [256, 8, 128], P(('replica', 'model'))
All inputs are finite; a program needn't handle non-finite values.
Results may differ from the reference program's by a relative error of at most 0.00217124.
Values are sent between devices in bfloat16 or wider.
A program may use at most 768 MiB of HBM per device.

```python
import jax
import jax.numpy as jnp
from jax import lax

D = 4096
QHEADS = 32
KVHEADS = 8
HEAD = 128
BATCH = 256
CONTEXT = 1024
GROUP_SIZE = QHEADS // KVHEADS
SCALE = HEAD ** -0.5


def draw_lengths(len_key):
    len_keys = jax.random.split(len_key, 2)
    lengths = jax.random.randint(len_keys[0], (BATCH,), 1, CONTEXT, dtype=jnp.int32)
    perm_order = jax.random.permutation(len_keys[1], BATCH)
    return lengths.at[perm_order[0]].set(CONTEXT - 1).at[perm_order[1]].set(1)


def setup_inputs(seed: int = 0, part: int = 0) -> dict:
    base_key = jax.random.key(seed)
    part_key = jax.random.fold_in(base_key, part)
    part_keys = jax.random.split(part_key, 3)
    weight_keys = jax.random.split(base_key, 4)
    query_cols = QHEADS * HEAD
    kv_cols = KVHEADS * HEAD
    tokens = jax.random.normal(part_keys[0], (BATCH, D), jnp.float32)
    w_query = jax.random.normal(weight_keys[0], (D, query_cols), jnp.float32) * D ** -0.5
    w_key = jax.random.normal(weight_keys[1], (D, kv_cols), jnp.float32) * (3.0 * D ** -0.5)
    w_value = jax.random.normal(weight_keys[2], (D, kv_cols), jnp.float32) * D ** -0.5
    w_out = jax.random.normal(weight_keys[3], (query_cols, D), jnp.float32) * query_cols ** -0.5
    key_cache = 3.0 * jax.random.normal(part_keys[1], (BATCH, KVHEADS, CONTEXT, HEAD), jnp.float32)
    value_cache = jax.random.normal(part_keys[2], (BATCH, KVHEADS, CONTEXT, HEAD), jnp.float32)
    lengths = draw_lengths(jax.random.fold_in(part_key, 3))
    return {
        "tokens": tokens.astype(jnp.bfloat16),
        "w_query": w_query.astype(jnp.bfloat16),
        "w_key": w_key.astype(jnp.bfloat16),
        "w_value": w_value.astype(jnp.bfloat16),
        "w_out": w_out.astype(jnp.bfloat16),
        "key_cache": key_cache.astype(jnp.bfloat16),
        "value_cache": value_cache.astype(jnp.bfloat16),
        "lengths": lengths,
    }


def reference(tokens, w_query, w_key, w_value, w_out, key_cache, value_cache, lengths):
    queries = jnp.dot(tokens, w_query, preferred_element_type=jnp.float32).astype(jnp.bfloat16)
    queries = queries.reshape(BATCH, KVHEADS, GROUP_SIZE, HEAD)
    key_new = jnp.dot(tokens, w_key, preferred_element_type=jnp.float32).astype(jnp.bfloat16)
    key_new = key_new.reshape(BATCH, KVHEADS, HEAD)
    value_new = jnp.dot(tokens, w_value, preferred_element_type=jnp.float32).astype(jnp.bfloat16)
    value_new = value_new.reshape(BATCH, KVHEADS, HEAD)

    def one_sequence(item):
        q_seq, key_seq, value_seq, key_last, value_last, seq_len = item
        q_wide = q_seq.astype(jnp.float32)
        scores = jnp.einsum("grd,gtd->grt", q_wide, key_seq.astype(jnp.float32)) * SCALE
        score_new = jnp.einsum("grd,gd->gr", q_wide, key_last.astype(jnp.float32)) * SCALE
        positions = jnp.arange(CONTEXT)
        scores = jnp.where(positions < seq_len, scores, -jnp.inf)
        score_max = jnp.maximum(jnp.max(scores, axis=-1), score_new)
        weights = jnp.exp(scores - score_max[..., None])
        weight_new = jnp.exp(score_new - score_max)
        denom_sum = jnp.sum(weights, axis=-1) + weight_new
        weighted_sum = jnp.einsum("grt,gtd->grd", weights.astype(jnp.bfloat16).astype(jnp.float32), value_seq.astype(jnp.float32))
        weighted_sum = weighted_sum + weight_new.astype(jnp.bfloat16).astype(jnp.float32)[..., None] * value_last.astype(jnp.float32)[:, None, :]
        return (weighted_sum / denom_sum[..., None]).astype(jnp.bfloat16)

    attended = lax.map(one_sequence, (queries, key_cache, value_cache, key_new, value_new, lengths))
    mixed_sum = jnp.dot(attended.reshape(BATCH, QHEADS * HEAD), w_out, preferred_element_type=jnp.float32)
    out_tokens = (tokens.astype(jnp.float32) + mixed_sum).astype(jnp.bfloat16)
    return (out_tokens, key_new, value_new)
```

```python
import functools

import jax
import jax.numpy as jnp
from jax import lax
from jax.experimental import pallas as pl
from jax.experimental.pallas import tpu as pltpu
from jax.sharding import PartitionSpec as P

CORES = 2
ROW_TILE = 16
SEQ_STEP = 4
MESH = pl.DeviceIdType.MESH
F32 = jnp.float32
BF16 = jnp.bfloat16


def remote(src, dst, send_sem, recv_sem, head_pos, model_pos):
    return pltpu.make_async_remote_copy(
        src_ref=src,
        dst_ref=dst,
        send_sem=send_sem,
        recv_sem=recv_sem,
        device_id={"heads": head_pos, "model": model_pos},
        device_id_type=MESH,
    )


def step_kernel(
    dims,
    tokens, w_query, w_key, w_value, w_out, key_cache, value_cache, lengths,
    out, key_out, value_out,
    tok_v, wq_v, wkv_v, kbuf, vbuf, wo_v, q_send, q_recv, q_wide, new_v, new_wide, p_v, l_v, o_wide, o_v, out_v,
    load_sem, wkv_sem, kv_sem, own_sem, q_ss, q_rs, w_ss, w_rs, f_ss, f_rs, n_ss, n_rs, a_ss, a_rs, g_ss, g_rs, d_ss, d_rs, s_sem,
):
    H, NX = dims["heads"], dims["chips_x"]
    M = NX * CORES
    lr, T, dh, D = dims["rows"], dims["context"], dims["head_dim"], dims["width"]
    kvs, qs, gs = dims["kv_shard"], dims["q_shard"], dims["group"]
    cols = dims["cols"]
    kvw = kvs * dh
    qw = qs * dh
    n_load = dims["n_load"]
    kc = D // n_load
    h = lax.axis_index("heads")
    m = lax.axis_index("model")
    x = m // CORES
    c = m % CORES
    partner = x * CORES + (1 - c)
    chip = h * NX + x
    R = H

    tok_loads, wq_loads = [], []
    for i in range(n_load):
        a = pltpu.make_async_copy(tokens.at[:, :, :, pl.ds(i * kc, kc)], tok_v.at[:, :, :, pl.ds(i * kc, kc)], load_sem.at[2 * i])
        b = pltpu.make_async_copy(w_query.at[pl.ds(i * kc, kc), :], wq_v.at[pl.ds(i * kc, kc), :], load_sem.at[2 * i + 1])
        a.start()
        b.start()
        tok_loads.append(a)
        wq_loads.append(b)
    kv_cols = pl.ds(pl.multiple_of(h * kvw, kvw), kvw)
    wk_load = pltpu.make_async_copy(w_key.at[:, kv_cols], wkv_v.at[0], wkv_sem.at[0])
    wv_load = pltpu.make_async_copy(w_value.at[:, kv_cols], wkv_v.at[1], wkv_sem.at[1])
    wk_load.start()
    wv_load.start()
    my_cols = pl.ds(pl.multiple_of(chip * cols, cols), cols)
    own_load = pltpu.make_async_copy(w_out.at[:, my_cols], wo_v.at[h * M + m], own_sem)
    own_load.start()

    steps = lr // SEQ_STEP

    def k_load(i):
        return pltpu.make_async_copy(
            key_cache.at[pl.ds(i * SEQ_STEP, SEQ_STEP), pl.ds(h * kvs, kvs)], kbuf.at[pl.ds(i * SEQ_STEP, SEQ_STEP)], kv_sem.at[0, i])

    def v_load(i):
        return pltpu.make_async_copy(
            value_cache.at[pl.ds(i * SEQ_STEP, SEQ_STEP), pl.ds(h * kvs, kvs)], vbuf.at[pl.ds(i * SEQ_STEP, SEQ_STEP)], kv_sem.at[1, i])

    for i in range(steps):
        k_load(i).start()
        v_load(i).start()

    barrier = pltpu.get_barrier_semaphore()
    peers = 0
    for dy in range(H):
        for dx in range(NX):
            if dx or dy:
                pl.semaphore_signal(barrier, inc=1, device_id={"heads": (h + dy) % H, "model": ((x + dx) % NX) * CORES + c}, device_id_type=MESH)
                peers += 1
    for dx in range(NX):
        pl.semaphore_signal(barrier, inc=1, device_id={"heads": h, "model": ((x + dx) % NX) * CORES + (1 - c)}, device_id_type=MESH)
        peers += 1

    acc = jnp.zeros((M * lr, dh), F32)
    for i in range(n_load):
        tok_loads[i].wait()
        wq_loads[i].wait()
        t = tok_v[:, :, :, pl.ds(i * kc, kc)].reshape(M * lr, kc)
        acc = acc + jnp.dot(t, wq_v[pl.ds(i * kc, kc), :], preferred_element_type=F32)
    q_send[...] = acc.astype(BF16).reshape(M, lr, dh)

    pl.semaphore_wait(barrier, peers)

    q_copies = []
    for k in sorted(range(1, M), key=lambda k: -min(k, M - k)):
        to = (m + k) % M
        cp = remote(q_send.at[to], q_recv.at[m], q_ss.at[k], q_rs.at[k], h, to)
        cp.start()
        q_copies.append(cp)

    w_copies = []
    order = [(dx, dy) for dx in range(NX) for dy in range(H) if dx or dy]
    order.sort(key=lambda d: -(min(d[0], NX - d[0]) + min(d[1], H - d[1])))
    for dx, dy in order:
        tx, ty = (x + dx) % NX, (h + dy) % H
        to_cols = pl.ds(pl.multiple_of((ty * NX + tx) * cols, cols), cols)
        cp = remote(w_out.at[:, to_cols], wo_v.at[h * M + m], w_ss.at[dy * NX + dx], w_rs.at[dy * NX + dx], ty, tx * CORES + c)
        cp.start()
        w_copies.append(cp)

    q_recv[m] = q_send[m]

    own_tok = tok_v[x, c]
    wk_load.wait()
    key_new = jnp.dot(own_tok, wkv_v[0], preferred_element_type=F32).astype(BF16)
    wv_load.wait()
    value_new = jnp.dot(own_tok, wkv_v[1], preferred_element_type=F32).astype(BF16)
    new_v[0, :, kv_cols] = key_new
    new_v[1, :, kv_cols] = value_new
    for g in range(kvs):
        new_wide[pl.ds(g * lr, lr), :] = key_new[:, g * dh:(g + 1) * dh].astype(F32)
        new_wide[pl.ds((kvs + g) * lr, lr), :] = value_new[:, g * dh:(g + 1) * dh].astype(F32)

    def new_block(pos):
        return new_v.at[:, :, pl.ds(pl.multiple_of(pos * kvw, kvw), kvw)]

    n_copies = []
    for k in range(1, H):
        cp = remote(new_block(h), new_block(h), n_ss.at[k], n_rs.at[k], (h + k) % H, m)
        cp.start()
        n_copies.append(cp)

    for k in range(1, M):
        frm = (m + M - k) % M
        remote(q_recv.at[frm], q_recv.at[frm], q_ss.at[k], q_rs.at[k], h, m).wait_recv()
    q_wide[...] = q_recv[...].astype(F32).reshape(M * lr, dh)

    scale = dh ** -0.5
    row = lax.broadcasted_iota(jnp.int32, (qs, dh), 0)
    pos = lax.broadcasted_iota(jnp.int32, (qs, T), 1)
    tile_row = lax.broadcasted_iota(jnp.int32, (ROW_TILE, dh), 0)

    def with_new(buf, which, b):
        parts = []
        fresh = new_wide[pl.ds(which * kvs * lr + b, kvs, stride=lr), :]
        for g in range(kvs):
            tail = buf[b, g, pl.ds(T - ROW_TILE, ROW_TILE), :].astype(F32)
            tail = jnp.where(tile_row == ROW_TILE - 1, jnp.broadcast_to(fresh[g:g + 1], (ROW_TILE, dh)), tail).astype(BF16)
            parts.append(jnp.concatenate([buf[b, g, pl.ds(0, T - ROW_TILE), :], tail], axis=0))
        return jnp.concatenate(parts, axis=1)

    def scores_of(i):
        for s in range(SEQ_STEP):
            b = i * SEQ_STEP + s
            qb = q_wide[pl.ds(b, qs, stride=lr), :]
            qb = jnp.concatenate([jnp.where(row // gs == g, qb, 0.0) for g in range(kvs)], axis=1).astype(BF16)
            sc = lax.dot_general(qb, with_new(kbuf, 0, b), (((1,), (1,)), ((), ())), preferred_element_type=F32) * scale
            sc = jnp.where(jnp.logical_or(pos < lengths[b], pos == T - 1), sc, -jnp.inf)
            top = jnp.max(sc, axis=1, keepdims=True)
            p = jnp.exp(sc - top)
            l_v[i % 2, s] = jnp.broadcast_to(jnp.sum(p, axis=1, keepdims=True), (qs, dh))
            p_v[i % 2, s] = p.astype(BF16)

    def values_of(i):
        for s in range(SEQ_STEP):
            b = i * SEQ_STEP + s
            wide = jnp.dot(p_v[i % 2, s], with_new(vbuf, 1, b), preferred_element_type=F32)
            o = wide[:, :dh]
            for g in range(1, kvs):
                o = jnp.where(row // gs == g, wide[:, g * dh:(g + 1) * dh], o)
            o_wide[pl.ds(b * qs, qs), :] = o / l_v[i % 2, s]

    def peer_first(k):
        return (h + k * c) % H, ((x + k * (1 - c)) % NX) * CORES + c

    def peer_second(k):
        return (h + k * (1 - c)) % H, ((x + k * c) % NX) * CORES + c

    def source(k1, k2):
        return (h + 2 * R - k1 * c - k2 * (1 - c)) % H, (x + 2 * R - k1 * (1 - c) - k2 * c) % NX

    hops = [k for k in range(1, R)]
    hops.sort(key=lambda k: -min(k, R - k))

    def o_block(g, sy, sx):
        return o_v.at[sx, pl.ds(g * ROW_TILE, ROW_TILE), pl.ds(pl.multiple_of(sy * qw, qw), qw)]

    def a_send_own(g):
        for j in range(qs):
            o_v[x, pl.ds(g * ROW_TILE, ROW_TILE), pl.ds(pl.multiple_of(h * qw + j * dh, dh), dh)] = (
                o_wide[pl.ds(g * ROW_TILE * qs + j, ROW_TILE, stride=qs), :].astype(BF16))
        blk = o_block(g, h, x)
        for k in hops:
            remote(blk, blk, a_ss.at[g, k * R], a_rs.at[g, k * R], *peer_first(k)).start()
        for k in hops:
            remote(blk, blk, a_ss.at[g, k], a_rs.at[g, k], *peer_second(k)).start()

    def a_forward(g):
        for k1 in (*hops[1:], hops[0]):
            blk = o_block(g, *source(k1, 0))
            remote(blk, blk, a_ss.at[g, k1 * R], a_rs.at[g, k1 * R], h, m).wait_recv()
            for k2 in hops:
                remote(blk, blk, a_ss.at[g, k1 * R + k2], a_rs.at[g, k1 * R + k2], *peer_second(k2)).start()

    groups = lr // ROW_TILE
    per_group = ROW_TILE // SEQ_STEP

    k_load(0).wait()
    scores_of(0)

    def body(i, carry):
        for g in range(groups - 1):
            @pl.when(i == (g + 1) * per_group + 1)
            def _():
                a_send_own(g)
        k_load(i).wait()
        v_load(i - 1).wait()
        scores_of(i)
        values_of(i - 1)
        return carry

    lax.fori_loop(1, steps, body, 0)
    v_load(steps - 1).wait()
    values_of(steps - 1)
    a_send_own(groups - 1)
    for g in range(groups - 1):
        a_forward(g)

    own_load.wait()
    def wo_forward(sy, sx, idx):
        blk = wo_v.at[sy * M + sx * CORES + c]
        remote(blk, blk, f_ss.at[idx], f_rs.at[idx], h, partner).start()

    wo_forward(h, x, 0)
    a_forward(groups - 1)
    for dx, dy in order:
        sx, sy = (x + NX - dx) % NX, (h + H - dy) % H
        blk = wo_v.at[sy * M + sx * CORES + c]
        remote(blk, blk, w_ss.at[dy * NX + dx], w_rs.at[dy * NX + dx], h, m).wait_recv()
        wo_forward(sy, sx, dy * NX + dx)

    def new_store(which, dst):
        return pltpu.make_async_copy(new_v.at[which], dst, s_sem.at[which])

    for k in range(1, H):
        blk = new_block((h + H - k) % H)
        remote(blk, blk, n_ss.at[k], n_rs.at[k], h, m).wait_recv()
    new_store(0, key_out).start()
    new_store(1, value_out).start()

    for dx, dy in [(0, 0)] + order:
        sx, sy = (x + NX - dx) % NX, (h + H - dy) % H
        blk = wo_v.at[sy * M + sx * CORES + (1 - c)]
        remote(blk, blk, f_ss.at[dy * NX + dx], f_rs.at[dy * NX + dx], h, m).wait_recv()
    for g in range(groups):
        for k1 in range(R):
            for k2 in range(1, R):
                blk = o_block(g, *source(k1, k2))
                remote(blk, blk, a_ss.at[g, k1 * R + k2], a_rs.at[g, k1 * R + k2], h, m).wait_recv()

    mixed = jnp.dot(o_v[...].reshape(NX * lr, H * qw), wo_v[...].reshape(H * M * dh, cols), preferred_element_type=F32)
    mixed = tok_v[:, c, :, my_cols].astype(F32) + mixed.reshape(NX, lr, cols)
    out_v[:, c, :, my_cols] = mixed.astype(BF16)

    def out_block(core, sy, sx):
        return out_v.at[:, core, :, pl.ds(pl.multiple_of((sy * NX + sx) * cols, cols), cols)]

    def d_forward(k1, k2):
        blk = out_block(c, *source(k1, k2))
        remote(blk, blk, d_ss.at[k1 * R + k2], d_rs.at[k1 * R + k2], h, partner).start()

    blk = out_block(c, h, x)
    for k in hops:
        remote(blk, blk, g_ss.at[k * R], g_rs.at[k * R], *peer_first(k)).start()
    for k in hops:
        remote(blk, blk, g_ss.at[k], g_rs.at[k], *peer_second(k)).start()
    d_forward(0, 0)
    for k1 in (*hops[1:], hops[0]):
        blk = out_block(c, *source(k1, 0))
        remote(blk, blk, g_ss.at[k1 * R], g_rs.at[k1 * R], h, m).wait_recv()
        for k2 in hops:
            remote(blk, blk, g_ss.at[k1 * R + k2], g_rs.at[k1 * R + k2], *peer_second(k2)).start()
        d_forward(k1, 0)
    for k1 in range(R):
        for k2 in range(1, R):
            blk = out_block(c, *source(k1, k2))
            remote(blk, blk, g_ss.at[k1 * R + k2], g_rs.at[k1 * R + k2], h, m).wait_recv()
            d_forward(k1, k2)
    own_store = pltpu.make_async_copy(out_v.at[:, c], out.at[:, c], s_sem.at[2])
    own_store.start()
    for k1 in range(R):
        for k2 in range(R):
            sy, sx = (h + 2 * R - k1 * (1 - c) - k2 * c) % H, (x + 2 * R - k1 * c - k2 * (1 - c)) % NX
            blk = out_block(1 - c, sy, sx)
            remote(blk, blk, d_ss.at[k1 * R + k2], d_rs.at[k1 * R + k2], h, m).wait_recv()
    other_store = pltpu.make_async_copy(out_v.at[:, 1 - c], out.at[:, 1 - c], s_sem.at[3])
    other_store.start()

    for cp in q_copies + w_copies + n_copies:
        cp.wait_send()
    for idx in range(H * NX):
        blk = wo_v.at[0]
        remote(blk, blk, f_ss.at[idx], f_rs.at[idx], h, m).wait_send()
    for g in range(groups):
        for idx in range(1, R * R):
            blk = o_block(g, h, x)
            remote(blk, blk, a_ss.at[g, idx], a_rs.at[g, idx], h, m).wait_send()
    for idx in range(R * R):
        blk = out_block(c, h, x)
        if idx:
            remote(blk, blk, g_ss.at[idx], g_rs.at[idx], h, m).wait_send()
        remote(blk, blk, d_ss.at[idx], d_rs.at[idx], h, m).wait_send()
    new_store(0, key_out).wait()
    new_store(1, value_out).wait()
    own_store.wait()
    other_store.wait()


def solution(mesh):
    heads_count = mesh.shape["heads"]
    model_count = mesh.shape["model"]

    def local_step(tokens, w_query, w_key, w_value, w_out, key_cache, value_cache, lengths):
        batch_all, width = tokens.shape
        rows, kv_count, context, head_dim = key_cache.shape
        chips_x = model_count // CORES
        q_shard = model_count * (w_query.shape[1] // head_dim)
        group = q_shard * heads_count // kv_count
        kv_shard = q_shard // group
        cols = width // (heads_count * chips_x)
        dims = dict(heads=heads_count, chips_x=chips_x, rows=rows, context=context, head_dim=head_dim, width=width,
                    kv_shard=kv_shard, q_shard=q_shard, group=group, cols=cols, n_load=4)
        assert heads_count == chips_x and q_shard == model_count
        steps = rows // SEQ_STEP
        groups = rows // ROW_TILE
        ring = heads_count
        any_spec = pl.BlockSpec(memory_space=pl.ANY)
        dma = pltpu.SemaphoreType.DMA
        out, key_new, value_new = pl.pallas_call(
            functools.partial(step_kernel, dims),
            out_shape=(
                jax.ShapeDtypeStruct((chips_x, CORES, rows, width), BF16),
                jax.ShapeDtypeStruct((rows, kv_count * head_dim), BF16),
                jax.ShapeDtypeStruct((rows, kv_count * head_dim), BF16),
            ),
            in_specs=[any_spec] * 7 + [pl.BlockSpec(memory_space=pltpu.SMEM)],
            out_specs=(any_spec,) * 3,
            scratch_shapes=[
                pltpu.VMEM((chips_x, CORES, rows, width), BF16),
                pltpu.VMEM((width, head_dim), BF16),
                pltpu.VMEM((2, width, kv_shard * head_dim), BF16),
                pltpu.VMEM((rows, kv_shard, context, head_dim), BF16),
                pltpu.VMEM((rows, kv_shard, context, head_dim), BF16),
                pltpu.VMEM((heads_count * model_count, head_dim, cols), BF16),
                pltpu.VMEM((model_count, rows, head_dim), BF16),
                pltpu.VMEM((model_count, rows, head_dim), BF16),
                pltpu.VMEM((model_count * rows, head_dim), F32),
                pltpu.VMEM((2, rows, kv_count * head_dim), BF16),
                pltpu.VMEM((2 * kv_shard * rows, head_dim), F32),
                pltpu.VMEM((2, SEQ_STEP, q_shard, context), BF16),
                pltpu.VMEM((2, SEQ_STEP, q_shard, head_dim), F32),
                pltpu.VMEM((rows * q_shard, head_dim), F32),
                pltpu.VMEM((chips_x, rows, heads_count * q_shard * head_dim), BF16),
                pltpu.VMEM((chips_x, CORES, rows, width), BF16),
                dma((8,)),
                dma((2,)),
                dma((2, steps)),
                dma,
                dma((model_count,)),
                dma((model_count,)),
                dma((ring * ring,)),
                dma((ring * ring,)),
                dma((ring * ring,)),
                dma((ring * ring,)),
                dma((ring,)),
                dma((ring,)),
                dma((groups, ring * ring)),
                dma((groups, ring * ring)),
                dma((ring * ring,)),
                dma((ring * ring,)),
                dma((ring * ring,)),
                dma((ring * ring,)),
                dma((4,)),
            ],
            compiler_params=pltpu.CompilerParams(
                collective_id=0, has_side_effects=True, vmem_limit_bytes=60 * 1024 * 1024
            ),
            name="decode_step",
        )(
            tokens.reshape(chips_x, CORES, rows, width), w_query, w_key, w_value, w_out, key_cache, value_cache, lengths
        )
        new_shape = (rows, kv_count, head_dim)
        return out.reshape(batch_all, width), key_new.reshape(new_shape), value_new.reshape(new_shape)

    cache_spec = P(("replica", "model"), None, None, None)
    new_spec = P(("replica", "model"), None, None)
    return jax.shard_map(
        local_step,
        mesh=mesh,
        in_specs=(P("replica", None), P(None, ("heads", "model")), P(None, None), P(None, None), P(("heads", "model"), None), cache_spec, cache_spec, P(("replica", "model"))),
        out_specs=(P("replica", None), new_spec, new_spec),
        check_vma=False,
    )
```

```python
import functools

import jax
import jax.numpy as jnp
from jax import lax
from jax.experimental import pallas as pl
from jax.experimental.pallas import tpu as pltpu
from jax.sharding import PartitionSpec as P

CORES = 2
ROW_TILE = 16
SEQ_STEP = 4
AHEAD = 4
MESH = pl.DeviceIdType.MESH
F32 = jnp.float32
BF16 = jnp.bfloat16


def remote(src, dst, send_sem, recv_sem, head_pos, model_pos):
    return pltpu.make_async_remote_copy(
        src_ref=src,
        dst_ref=dst,
        send_sem=send_sem,
        recv_sem=recv_sem,
        device_id={"heads": head_pos, "model": model_pos},
        device_id_type=MESH,
    )


def step_kernel(
    dims,
    tokens, w_query, w_key, w_value, w_out, key_cache, value_cache, lengths,
    out_v, fresh_v,
    tok_v, wq_v, wkv_v, kbuf, vbuf, wo_v, q_send, q_recv, q_wide, new_v, new_wide, p_v, l_v, o_wide, o_v,
    load_sem, wkv_sem, kv_sem, own_sem, q_ss, q_rs, w_ss, w_rs, f_ss, f_rs, n_ss, n_rs, a_ss, a_rs, g_ss, g_rs, d_ss, d_rs,
):
    H, NX = dims["heads"], dims["chips_x"]
    M = NX * CORES
    lr, T, dh, D = dims["rows"], dims["context"], dims["head_dim"], dims["width"]
    kvs, qs, gs = dims["kv_shard"], dims["q_shard"], dims["group"]
    cols = dims["cols"]
    kvw = kvs * dh
    qw = qs * dh
    n_load = dims["n_load"]
    kc = D // n_load
    h = lax.axis_index("heads")
    m = lax.axis_index("model")
    x = m // CORES
    c = m % CORES
    partner = x * CORES + (1 - c)
    chip = h * NX + x
    R = H

    tok_loads, wq_loads = [], []
    for i in range(n_load):
        a = pltpu.make_async_copy(tokens.at[:, :, :, pl.ds(i * kc, kc)], tok_v.at[:, :, :, pl.ds(i * kc, kc)], load_sem.at[2 * i])
        b = pltpu.make_async_copy(w_query.at[pl.ds(i * kc, kc), :], wq_v.at[pl.ds(i * kc, kc), :], load_sem.at[2 * i + 1])
        a.start()
        b.start()
        tok_loads.append(a)
        wq_loads.append(b)
    kv_cols = pl.ds(pl.multiple_of(h * kvw, kvw), kvw)
    wk_load = pltpu.make_async_copy(w_key.at[:, kv_cols], wkv_v.at[0], wkv_sem.at[0])
    wv_load = pltpu.make_async_copy(w_value.at[:, kv_cols], wkv_v.at[1], wkv_sem.at[1])
    my_cols = pl.ds(pl.multiple_of(chip * cols, cols), cols)
    own_load = pltpu.make_async_copy(w_out.at[:, my_cols], wo_v.at[h * M + m], own_sem)
    own_load.start()

    steps = lr // SEQ_STEP

    def k_load(i):
        return pltpu.make_async_copy(
            key_cache.at[pl.ds(i * SEQ_STEP, SEQ_STEP), pl.ds(h * kvs, kvs)], kbuf.at[pl.ds(i * SEQ_STEP, SEQ_STEP)], kv_sem.at[0, i])

    def v_load(i):
        return pltpu.make_async_copy(
            value_cache.at[pl.ds(i * SEQ_STEP, SEQ_STEP), pl.ds(h * kvs, kvs)], vbuf.at[pl.ds(i * SEQ_STEP, SEQ_STEP)], kv_sem.at[1, i])

    def kv_start(i):
        k_load(i).start()
        v_load(i).start()

    barrier = pltpu.get_barrier_semaphore()
    peers = 0
    for dy in range(H):
        for dx in range(NX):
            if dx or dy:
                pl.semaphore_signal(barrier, inc=1, device_id={"heads": (h + dy) % H, "model": ((x + dx) % NX) * CORES + c}, device_id_type=MESH)
                peers += 1
    for dx in range(NX):
        pl.semaphore_signal(barrier, inc=1, device_id={"heads": h, "model": ((x + dx) % NX) * CORES + (1 - c)}, device_id_type=MESH)
        peers += 1

    with jax.named_scope("q_proj"):
        acc = jnp.zeros((M * lr, dh), F32)
        for i in range(n_load):
            tok_loads[i].wait()
            wq_loads[i].wait()
            if i == n_load - 2:
                wk_load.start()
                wv_load.start()
                kv_start(0)
            t = tok_v[:, :, :, pl.ds(i * kc, kc)].reshape(M * lr, kc)
            acc = acc + jnp.dot(t, wq_v[pl.ds(i * kc, kc), :], preferred_element_type=F32)
        q_send[...] = acc.astype(BF16).reshape(M, lr, dh)

    with jax.named_scope("barrier"):
        pl.semaphore_wait(barrier, peers)

    q_copies = []
    for k in sorted(range(1, M), key=lambda k: -min(k, M - k)):
        to = (m + k) % M
        cp = remote(q_send.at[to], q_recv.at[m], q_ss.at[k], q_rs.at[k], h, to)
        cp.start()
        q_copies.append(cp)

    w_copies = []
    order = [(dx, dy) for dx in range(NX) for dy in range(H) if dx or dy]
    order.sort(key=lambda d: -(min(d[0], NX - d[0]) + min(d[1], H - d[1])))
    for dx, dy in order:
        tx, ty = (x + dx) % NX, (h + dy) % H
        to_cols = pl.ds(pl.multiple_of((ty * NX + tx) * cols, cols), cols)
        cp = remote(w_out.at[:, to_cols], wo_v.at[h * M + m], w_ss.at[dy * NX + dx], w_rs.at[dy * NX + dx], ty, tx * CORES + c)
        cp.start()
        w_copies.append(cp)

    kv_start(1)
    with jax.named_scope("kv_new"):
        q_recv[m] = q_send[m]

        own_tok = tok_v[x, c]
        wk_load.wait()
        key_new = jnp.dot(own_tok, wkv_v[0], preferred_element_type=F32).astype(BF16)
        wv_load.wait()
        value_new = jnp.dot(own_tok, wkv_v[1], preferred_element_type=F32).astype(BF16)
        new_v[0, :, kv_cols] = key_new
        new_v[1, :, kv_cols] = value_new
        for g in range(kvs):
            new_wide[pl.ds(g * lr, lr), :] = key_new[:, g * dh:(g + 1) * dh].astype(F32)
            new_wide[pl.ds((kvs + g) * lr, lr), :] = value_new[:, g * dh:(g + 1) * dh].astype(F32)

    def new_block(pos):
        return new_v.at[:, :, pl.ds(pl.multiple_of(pos * kvw, kvw), kvw)]

    n_copies = []
    for k in range(1, H):
        cp = remote(new_block(h), new_block(h), n_ss.at[k], n_rs.at[k], (h + k) % H, m)
        cp.start()
        n_copies.append(cp)

    for i in range(2, AHEAD):
        kv_start(i)
    with jax.named_scope("q_wait"):
        for k in range(1, M):
            frm = (m + M - k) % M
            remote(q_recv.at[frm], q_recv.at[frm], q_ss.at[k], q_rs.at[k], h, m).wait_recv()
        q_wide[...] = q_recv[...].astype(F32).reshape(M * lr, dh)

    scale = dh ** -0.5
    row = lax.broadcasted_iota(jnp.int32, (qs, dh), 0)
    pos = lax.broadcasted_iota(jnp.int32, (qs, T), 1)
    tile_row = lax.broadcasted_iota(jnp.int32, (ROW_TILE, dh), 0)

    def with_new(buf, which, b):
        parts = []
        fresh = new_wide[pl.ds(which * kvs * lr + b, kvs, stride=lr), :]
        for g in range(kvs):
            tail = buf[b, g, pl.ds(T - ROW_TILE, ROW_TILE), :].astype(F32)
            tail = jnp.where(tile_row == ROW_TILE - 1, jnp.broadcast_to(fresh[g:g + 1], (ROW_TILE, dh)), tail).astype(BF16)
            parts.append(jnp.concatenate([buf[b, g, pl.ds(0, T - ROW_TILE), :], tail], axis=0))
        return jnp.concatenate(parts, axis=1)

    def scores_of(i):
        for s in range(SEQ_STEP):
            b = i * SEQ_STEP + s
            qb = q_wide[pl.ds(b, qs, stride=lr), :]
            qb = jnp.concatenate([jnp.where(row // gs == g, qb, 0.0) for g in range(kvs)], axis=1).astype(BF16)
            sc = lax.dot_general(qb, with_new(kbuf, 0, b), (((1,), (1,)), ((), ())), preferred_element_type=F32) * scale
            sc = jnp.where(jnp.logical_or(pos < lengths[b], pos == T - 1), sc, -jnp.inf)
            top = jnp.max(sc, axis=1, keepdims=True)
            p = jnp.exp(sc - top)
            l_v[i % 2, s] = jnp.broadcast_to(jnp.sum(p, axis=1, keepdims=True), (qs, dh))
            p_v[i % 2, s] = p.astype(BF16)

    def values_of(i):
        for s in range(SEQ_STEP):
            b = i * SEQ_STEP + s
            wide = jnp.dot(p_v[i % 2, s], with_new(vbuf, 1, b), preferred_element_type=F32)
            o = wide[:, :dh]
            for g in range(1, kvs):
                o = jnp.where(row // gs == g, wide[:, g * dh:(g + 1) * dh], o)
            o_wide[pl.ds(b * qs, qs), :] = o / l_v[i % 2, s]

    def place(k1, k2, core):
        return (h + 2 * R - k1 * core - k2 * (1 - core)) % H, (x + 2 * R - k1 * (1 - core) - k2 * core) % NX

    def neighbour(dim, step):
        along_y = c if dim == 0 else 1 - c
        return (h + R + step * along_y) % H, ((x + NX + step * (1 - along_y)) % NX) * CORES + c

    def sem_index(k1, k2, half):
        return (k1 * R + k2) * 2 + (half or 0)

    class Gather:
        def __init__(self, view, send_sems, recv_sems):
            self.view, self.send_sems, self.recv_sems, self.sent = view, send_sems, recv_sems, []

        def push(self, k1, k2, half, dim, step):
            mine = ((k1 - step) % R, k2) if dim == 0 else (k1, (k2 - step) % R)
            ref = self.view(*place(*mine, c), half)
            idx = sem_index(k1, k2, half)
            remote(ref, ref, self.send_sems(idx), self.recv_sems(idx), *neighbour(dim, step)).start()
            self.sent.append((idx, half))

        def arrive(self, k1, k2, half=None):
            ref = self.view(*place(k1, k2, c), half)
            idx = sem_index(k1, k2, half)
            remote(ref, ref, self.send_sems(idx), self.recv_sems(idx), h, m).wait_recv()

        def own(self):
            self.push(1, 0, None, 0, 1)
            self.push(3, 0, None, 0, -1)
            self.push(0, 1, None, 1, 1)
            self.push(0, 3, None, 1, -1)

        def stages(self, done=lambda k1, k2: None):
            def first(k1, half, step):
                self.arrive(k1, 0)
                self.push(2, 0, half, 0, step)
                self.push(k1, 1, None, 1, 1)
                self.push(k1, 3, None, 1, -1)
                done(k1, 0)

            def second(k1, k2, half, step):
                self.arrive(k1, k2)
                self.push(k1, 2, half, 1, step)
                done(k1, k2)

            def far():
                for half in range(2):
                    self.arrive(2, 0, half)
                    self.push(2, 1, half, 1, 1)
                    self.push(2, 3, half, 1, -1)
                done(2, 0)

            def far_second():
                self.arrive(2, 1, 0)
                self.push(2, 2, 0, 1, 1)
                self.arrive(2, 3, 1)
                self.push(2, 2, 1, 1, -1)
                self.arrive(2, 1, 1)
                done(2, 1)
                self.arrive(2, 3, 0)
                done(2, 3)

            def last(k1):
                self.arrive(k1, 2, 0)
                self.arrive(k1, 2, 1)
                done(k1, 2)

            return [
                lambda: first(1, 0, 1),
                lambda: first(3, 1, -1),
                lambda: second(0, 1, 0, 1),
                lambda: second(0, 3, 1, -1),
                far,
                lambda: second(1, 1, 0, 1),
                lambda: second(1, 3, 1, -1),
                lambda: second(3, 1, 0, 1),
                lambda: second(3, 3, 1, -1),
                lambda: last(0),
                far_second,
                lambda: last(1),
                lambda: last(3),
                lambda: last(2),
            ]

        def finish(self):
            for idx, half in self.sent:
                ref = self.view(h, x, half)
                remote(ref, ref, self.send_sems(idx), self.recv_sems(idx), h, m).wait_send()

    def o_view(g):
        def view(sy, sx, half):
            start, size = sy * qw, qw
            if half is not None:
                start, size = start + half * (qw // 2), qw // 2
            return o_v.at[sx, pl.ds(g * ROW_TILE, ROW_TILE), pl.ds(pl.multiple_of(start, size), size)]

        return view

    o_gathers = [
        Gather(o_view(g), functools.partial(lambda g, idx: a_ss.at[g, idx], g), functools.partial(lambda g, idx: a_rs.at[g, idx], g))
        for g in range(lr // ROW_TILE)
    ]

    def a_send_own(g):
        for j in range(qs):
            o_v[x, pl.ds(g * ROW_TILE, ROW_TILE), pl.ds(pl.multiple_of(h * qw + j * dh, dh), dh)] = (
                o_wide[pl.ds(g * ROW_TILE * qs + j, ROW_TILE, stride=qs), :].astype(BF16))
        o_gathers[g].own()

    groups = lr // ROW_TILE
    per_group = ROW_TILE // SEQ_STEP

    with jax.named_scope("first"):
        k_load(0).wait()
        scores_of(0)

    def body(i, carry):
        for g in range(groups - 1):
            @pl.when(i == (g + 1) * per_group + 1)
            def _():
                a_send_own(g)
        @pl.when(i + AHEAD - 1 < steps)
        def _():
            kv_start(i + AHEAD - 1)

        k_load(i).wait()
        v_load(i - 1).wait()
        scores_of(i)
        values_of(i - 1)
        return carry

    with jax.named_scope("attn"):
        lax.fori_loop(1, steps, body, 0)
        v_load(steps - 1).wait()
        values_of(steps - 1)

    with jax.named_scope("a_own"):
        a_send_own(groups - 1)

    def wo_forward(sy, sx, idx):
        blk = wo_v.at[sy * M + sx * CORES + c]
        remote(blk, blk, f_ss.at[idx], f_rs.at[idx], h, partner).start()

    with jax.named_scope("w_wait"):
        own_load.wait()
        wo_forward(h, x, 0)
        for dx, dy in order:
            sx, sy = (x + NX - dx) % NX, (h + H - dy) % H
            blk = wo_v.at[sy * M + sx * CORES + c]
            remote(blk, blk, w_ss.at[dy * NX + dx], w_rs.at[dy * NX + dx], h, m).wait_recv()
            wo_forward(sy, sx, dy * NX + dx)

    with jax.named_scope("new_wait"):
        for k in range(1, H):
            blk = new_block((h + H - k) % H)
            remote(blk, blk, n_ss.at[k], n_rs.at[k], h, m).wait_recv()
        for which in range(2):
            fresh_v[which] = new_v[which].astype(F32).reshape(fresh_v.shape[1:]).astype(BF16)

    o_stages = [gather.stages() for gather in o_gathers]
    for n, stage_group in enumerate(zip(*o_stages)):
        with jax.named_scope(f"a_stage#n={n}"):
            for stage in stage_group:
                stage()

    with jax.named_scope("f_wait"):
        for dx, dy in [(0, 0)] + order:
            sx, sy = (x + NX - dx) % NX, (h + H - dy) % H
            blk = wo_v.at[sy * M + sx * CORES + (1 - c)]
            remote(blk, blk, f_ss.at[dy * NX + dx], f_rs.at[dy * NX + dx], h, m).wait_recv()

    with jax.named_scope("proj"):
        mixed = jnp.dot(o_v[...].reshape(NX * lr, H * qw), wo_v[...].reshape(H * M * dh, cols), preferred_element_type=F32)
        mixed = tok_v[:, c, :, my_cols].astype(F32) + mixed.reshape(NX, lr, cols)
        out_v[:, c, :, my_cols] = mixed.astype(BF16)

    def out_view(core):
        def view(sy, sx, half):
            at = pl.ds(pl.multiple_of((sy * NX + sx) * cols, cols), cols)
            if half is None:
                return out_v.at[:, core, :, at]
            return out_v.at[pl.ds(half * (NX // 2), NX // 2), core, :, at]

        return view

    def d_copy(k1, k2, core):
        blk = out_view(core)(*place(k1, k2, core), None)
        return remote(blk, blk, d_ss.at[k1 * R + k2], d_rs.at[k1 * R + k2], h, partner)

    out_gather = Gather(out_view(c), lambda idx: g_ss.at[idx], lambda idx: g_rs.at[idx])
    out_gather.own()
    d_copy(0, 0, c).start()
    for n, stage in enumerate(out_gather.stages(lambda k1, k2: d_copy(k1, k2, c).start())):
        with jax.named_scope(f"g_stage#n={n}"):
            stage()
    with jax.named_scope("d_wait"):
        for k1 in range(R):
            for k2 in range(R):
                d_copy(k1, k2, 1 - c).wait_recv()

    with jax.named_scope("s_wait"):
        for cp in q_copies + w_copies + n_copies:
            cp.wait_send()
        for idx in range(H * NX):
            blk = wo_v.at[0]
            remote(blk, blk, f_ss.at[idx], f_rs.at[idx], h, m).wait_send()
        for gather in o_gathers:
            gather.finish()
        out_gather.finish()
        for k1 in range(R):
            for k2 in range(R):
                d_copy(k1, k2, c).wait_send()


def store_kernel(out_v, fresh_v, out, key_out, value_out, sems):
    copies = [
        pltpu.make_async_copy(out_v, out, sems.at[0]),
        pltpu.make_async_copy(fresh_v.at[0], key_out, sems.at[1]),
        pltpu.make_async_copy(fresh_v.at[1], value_out, sems.at[2]),
    ]
    for cp in copies:
        cp.start()
    for cp in copies:
        cp.wait()


def solution(mesh):
    heads_count = mesh.shape["heads"]
    model_count = mesh.shape["model"]

    def local_step(tokens, w_query, w_key, w_value, w_out, key_cache, value_cache, lengths):
        batch_all, width = tokens.shape
        rows, kv_count, context, head_dim = key_cache.shape
        chips_x = model_count // CORES
        q_shard = model_count * (w_query.shape[1] // head_dim)
        group = q_shard * heads_count // kv_count
        kv_shard = q_shard // group
        cols = width // (heads_count * chips_x)
        dims = dict(heads=heads_count, chips_x=chips_x, rows=rows, context=context, head_dim=head_dim, width=width,
                    kv_shard=kv_shard, q_shard=q_shard, group=group, cols=cols, n_load=4)
        assert heads_count == chips_x == 4 and q_shard == model_count
        steps = rows // SEQ_STEP
        groups = rows // ROW_TILE
        ring = heads_count
        any_spec = pl.BlockSpec(memory_space=pl.ANY)
        dma = pltpu.SemaphoreType.DMA
        vmem_spec = pl.BlockSpec(memory_space=pltpu.VMEM)
        out_tok, fresh = pl.pallas_call(
            functools.partial(step_kernel, dims),
            out_shape=(
                pltpu.VMEM((chips_x, CORES, rows, width), BF16),
                pltpu.VMEM((2, rows, kv_count, head_dim), BF16),
            ),
            in_specs=[any_spec] * 7 + [pl.BlockSpec(memory_space=pltpu.SMEM)],
            out_specs=(vmem_spec,) * 2,
            scratch_shapes=[
                pltpu.VMEM((chips_x, CORES, rows, width), BF16),
                pltpu.VMEM((width, head_dim), BF16),
                pltpu.VMEM((2, width, kv_shard * head_dim), BF16),
                pltpu.VMEM((rows, kv_shard, context, head_dim), BF16),
                pltpu.VMEM((rows, kv_shard, context, head_dim), BF16),
                pltpu.VMEM((heads_count * model_count, head_dim, cols), BF16),
                pltpu.VMEM((model_count, rows, head_dim), BF16),
                pltpu.VMEM((model_count, rows, head_dim), BF16),
                pltpu.VMEM((model_count * rows, head_dim), F32),
                pltpu.VMEM((2, rows, kv_count * head_dim), BF16),
                pltpu.VMEM((2 * kv_shard * rows, head_dim), F32),
                pltpu.VMEM((2, SEQ_STEP, q_shard, context), BF16),
                pltpu.VMEM((2, SEQ_STEP, q_shard, head_dim), F32),
                pltpu.VMEM((rows * q_shard, head_dim), F32),
                pltpu.VMEM((chips_x, rows, heads_count * q_shard * head_dim), BF16),
                dma((8,)),
                dma((2,)),
                dma((2, steps)),
                dma,
                dma((model_count,)),
                dma((model_count,)),
                dma((ring * ring,)),
                dma((ring * ring,)),
                dma((ring * ring,)),
                dma((ring * ring,)),
                dma((ring,)),
                dma((ring,)),
                dma((groups, ring * ring * 2)),
                dma((groups, ring * ring * 2)),
                dma((ring * ring * 2,)),
                dma((ring * ring * 2,)),
                dma((ring * ring,)),
                dma((ring * ring,)),
            ],
            compiler_params=pltpu.CompilerParams(
                collective_id=0, has_side_effects=True, vmem_limit_bytes=60 * 1024 * 1024
            ),
            name="decode_step",
        )(
            tokens.reshape(chips_x, CORES, rows, width), w_query, w_key, w_value, w_out, key_cache, value_cache, lengths
        )
        new_shape = jax.ShapeDtypeStruct((rows, kv_count, head_dim), BF16)
        out, key_new, value_new = pl.pallas_call(
            store_kernel,
            out_shape=(jax.ShapeDtypeStruct((chips_x, CORES, rows, width), BF16), new_shape, new_shape),
            in_specs=[any_spec] * 2,
            out_specs=(any_spec,) * 3,
            scratch_shapes=[dma((3,))],
            compiler_params=pltpu.CompilerParams(vmem_limit_bytes=1024 * 1024),
            name="store",
        )(out_tok, fresh)
        return out.reshape(batch_all, width), key_new, value_new

    cache_spec = P(("replica", "model"), None, None, None)
    new_spec = P(("replica", "model"), None, None)
    return jax.shard_map(
        local_step,
        mesh=mesh,
        in_specs=(P("replica", None), P(None, ("heads", "model")), P(None, None), P(None, None), P(("heads", "model"), None), cache_spec, cache_spec, P(("replica", "model"))),
        out_specs=(P("replica", None), new_spec, new_spec),
        check_vma=False,
    )
```

```python
import functools

import jax
import jax.numpy as jnp
from jax import lax
from jax.experimental import pallas as pl
from jax.experimental.pallas import tpu as pltpu
from jax.sharding import PartitionSpec as P

CORES = 2
ROW_TILE = 16
SEQ_STEP = 4
RELAY_STEP = 2
AHEAD = 4
MESH = pl.DeviceIdType.MESH
F32 = jnp.float32
BF16 = jnp.bfloat16


def remote(src, dst, send_sem, recv_sem, head_pos, model_pos):
    return pltpu.make_async_remote_copy(
        src_ref=src,
        dst_ref=dst,
        send_sem=send_sem,
        recv_sem=recv_sem,
        device_id={"heads": head_pos, "model": model_pos},
        device_id_type=MESH,
    )


def step_kernel(
    dims,
    tokens, w_query, w_key, w_value, w_out, key_cache, value_cache, lengths,
    out_v, fresh_v,
    tok_v, wq_v, wkv_v, kbuf, vbuf, wo_v, q_send, q_recv, q_wide, new_v, new_wide, p_v, l_v, o_wide, o_v, via_v,
    load_sem, wkv_sem, kv_sem, own_sem, q_sem, w_sem, via_sem, f_sem, n_sem, a_ss, a_rs, g_ss, g_rs, d_sem,
):
    H, NX = dims["heads"], dims["chips_x"]
    M = NX * CORES
    lr, T, dh, D = dims["rows"], dims["context"], dims["head_dim"], dims["width"]
    kvs, qs, gs = dims["kv_shard"], dims["q_shard"], dims["group"]
    cols = dims["cols"]
    kvw = kvs * dh
    qw = qs * dh
    n_load = dims["n_load"]
    kc = D // n_load
    h = lax.axis_index("heads")
    m = lax.axis_index("model")
    x = m // CORES
    c = m % CORES
    partner = x * CORES + (1 - c)
    chip = h * NX + x
    R = H

    tok_loads, wq_loads = [], []
    for i in range(n_load):
        a = pltpu.make_async_copy(tokens.at[:, :, :, pl.ds(i * kc, kc)], tok_v.at[:, :, :, pl.ds(i * kc, kc)], load_sem.at[2 * i])
        b = pltpu.make_async_copy(w_query.at[pl.ds(i * kc, kc), :], wq_v.at[pl.ds(i * kc, kc), :], load_sem.at[2 * i + 1])
        a.start()
        b.start()
        tok_loads.append(a)
        wq_loads.append(b)
    kv_cols = pl.ds(pl.multiple_of(h * kvw, kvw), kvw)
    wk_load = pltpu.make_async_copy(w_key.at[:, kv_cols], wkv_v.at[0], wkv_sem.at[0])
    wv_load = pltpu.make_async_copy(w_value.at[:, kv_cols], wkv_v.at[1], wkv_sem.at[1])
    my_cols = pl.ds(pl.multiple_of(chip * cols, cols), cols)
    own_load = pltpu.make_async_copy(w_out.at[:, my_cols], wo_v.at[chip, c], own_sem)
    own_load.start()

    steps = lr // SEQ_STEP

    def k_load(i):
        return pltpu.make_async_copy(
            key_cache.at[pl.ds(i * SEQ_STEP, SEQ_STEP), pl.ds(h * kvs, kvs)], kbuf.at[pl.ds(i * SEQ_STEP, SEQ_STEP)], kv_sem.at[0, i])

    def v_load(i):
        return pltpu.make_async_copy(
            value_cache.at[pl.ds(i * SEQ_STEP, SEQ_STEP), pl.ds(h * kvs, kvs)], vbuf.at[pl.ds(i * SEQ_STEP, SEQ_STEP)], kv_sem.at[1, i])

    def kv_start(i):
        k_load(i).start()
        v_load(i).start()

    barrier = pltpu.get_barrier_semaphore()
    peers = 0
    for dy in range(H):
        for dx in range(NX):
            if dx or dy:
                pl.semaphore_signal(barrier, inc=1, device_id={"heads": (h + dy) % H, "model": ((x + dx) % NX) * CORES + c}, device_id_type=MESH)
                peers += 1
    for dx in range(NX):
        pl.semaphore_signal(barrier, inc=1, device_id={"heads": h, "model": ((x + dx) % NX) * CORES + (1 - c)}, device_id_type=MESH)
        peers += 1

    with jax.named_scope("q_proj"):
        acc = jnp.zeros((M * lr, dh), F32)
        for i in range(n_load):
            tok_loads[i].wait()
            wq_loads[i].wait()
            if i == n_load - 2:
                wk_load.start()
                wv_load.start()
                kv_start(0)
            t = tok_v[:, :, :, pl.ds(i * kc, kc)].reshape(M * lr, kc)
            acc = acc + jnp.dot(t, wq_v[pl.ds(i * kc, kc), :], preferred_element_type=F32)
        q_send[...] = acc.astype(BF16).reshape(M, lr, dh)

    with jax.named_scope("barrier"):
        pl.semaphore_wait(barrier, peers)

    for k in sorted(range(1, M), key=lambda k: -min(k, M - k)):
        to = (m + k) % M
        remote(q_send.at[to], q_recv.at[m], q_sem.at[0], q_sem.at[1], h, to).start()

    relays = [((1, 0), (1, 0)), ((-1, 0), (-1, 1)), ((1, 0), (1, -1)), ((-1, -1), (-1, -1)), ((0, 1), (0, 1)), ((0, -1), (1, -1)), ((0, 1), (-1, 1))]
    directs = [(1, 0), (-1, 0), (0, 1), (0, -1), (1, 1), (-1, -1), (1, -1), (-1, 1)]

    def chip_at(dx, dy):
        return (h + H + dy) % H, (x + NX + dx) % NX

    def cols_of(sy, sx):
        return pl.ds(pl.multiple_of((sy * NX + sx) * cols, cols), cols)

    for n, ((ax, ay), (bx, by)) in enumerate(relays):
        vy, vx = chip_at(ax, ay)
        remote(w_out.at[:, cols_of(*chip_at(ax + bx, ay + by))], via_v.at[n], w_sem.at[0], via_sem, vy, vx * CORES + c).start()
    for dx, dy in directs:
        ty, tx = chip_at(dx, dy)
        remote(w_out.at[:, cols_of(ty, tx)], wo_v.at[chip, c], w_sem.at[0], w_sem.at[1], ty, tx * CORES + c).start()

    def blocks(n):
        return wo_v.at[pl.ds(0, n // 2)] if n % 2 == 0 else wo_v.at[pl.ds(0, n), 0]

    def w_relay():
        remote(via_v, via_v, w_sem.at[0], via_sem, h, m).wait_recv()
        for n, ((ax, ay), (bx, by)) in enumerate(relays):
            sy, sx = chip_at(-ax, -ay)
            ty, tx = chip_at(bx, by)
            remote(via_v.at[n], wo_v.at[sy * NX + sx, c], w_sem.at[0], w_sem.at[1], ty, tx * CORES + c).start()

    kv_start(1)
    with jax.named_scope("kv_new"):
        q_recv[m] = q_send[m]

        own_tok = tok_v[x, c]
        wk_load.wait()
        key_new = jnp.dot(own_tok, wkv_v[0], preferred_element_type=F32).astype(BF16)
        wv_load.wait()
        value_new = jnp.dot(own_tok, wkv_v[1], preferred_element_type=F32).astype(BF16)
        new_v[0, :, kv_cols] = key_new
        new_v[1, :, kv_cols] = value_new
        for g in range(kvs):
            new_wide[pl.ds(g * lr, lr), :] = key_new[:, g * dh:(g + 1) * dh].astype(F32)
            new_wide[pl.ds((kvs + g) * lr, lr), :] = value_new[:, g * dh:(g + 1) * dh].astype(F32)

    def new_block(pos):
        return new_v.at[:, :, pl.ds(pl.multiple_of(pos * kvw, kvw), kvw)]

    for k in range(1, H):
        remote(new_block(h), new_block(h), n_sem.at[0], n_sem.at[1], (h + k) % H, m).start()

    for i in range(2, AHEAD):
        kv_start(i)
    with jax.named_scope("q_wait"):
        others = q_recv.at[pl.ds(0, M - 1)]
        remote(others, others, q_sem.at[0], q_sem.at[1], h, m).wait_recv()
        q_wide[...] = q_recv[...].astype(F32).reshape(M * lr, dh)

    scale = dh ** -0.5
    row = lax.broadcasted_iota(jnp.int32, (qs, dh), 0)
    pos = lax.broadcasted_iota(jnp.int32, (qs, T), 1)
    tile_row = lax.broadcasted_iota(jnp.int32, (ROW_TILE, dh), 0)

    def with_new(buf, which, b):
        parts = []
        fresh = new_wide[pl.ds(which * kvs * lr + b, kvs, stride=lr), :]
        for g in range(kvs):
            tail = buf[b, g, pl.ds(T - ROW_TILE, ROW_TILE), :].astype(F32)
            tail = jnp.where(tile_row == ROW_TILE - 1, jnp.broadcast_to(fresh[g:g + 1], (ROW_TILE, dh)), tail).astype(BF16)
            parts.append(jnp.concatenate([buf[b, g, pl.ds(0, T - ROW_TILE), :], tail], axis=0))
        return jnp.concatenate(parts, axis=1)

    def scores_of(i):
        for s in range(SEQ_STEP):
            b = i * SEQ_STEP + s
            qb = q_wide[pl.ds(b, qs, stride=lr), :]
            qb = jnp.concatenate([jnp.where(row // gs == g, qb, 0.0) for g in range(kvs)], axis=1).astype(BF16)
            sc = lax.dot_general(qb, with_new(kbuf, 0, b), (((1,), (1,)), ((), ())), preferred_element_type=F32) * scale
            sc = jnp.where(jnp.logical_or(pos < lengths[b], pos == T - 1), sc, -jnp.inf)
            top = jnp.max(sc, axis=1, keepdims=True)
            p = jnp.exp(sc - top)
            l_v[i % 2, s] = jnp.broadcast_to(jnp.sum(p, axis=1, keepdims=True), (qs, dh))
            p_v[i % 2, s] = p.astype(BF16)

    def values_of(i):
        for s in range(SEQ_STEP):
            b = i * SEQ_STEP + s
            wide = jnp.dot(p_v[i % 2, s], with_new(vbuf, 1, b), preferred_element_type=F32)
            o = wide[:, :dh]
            for g in range(1, kvs):
                o = jnp.where(row // gs == g, wide[:, g * dh:(g + 1) * dh], o)
            o_wide[pl.ds(b * qs, qs), :] = o / l_v[i % 2, s]

    def place(k1, k2, core):
        return (h + 2 * R - k1 * core - k2 * (1 - core)) % H, (x + 2 * R - k1 * (1 - core) - k2 * core) % NX

    def neighbour(dim, step):
        along_y = c if dim == 0 else 1 - c
        return (h + R + step * along_y) % H, ((x + NX + step * (1 - along_y)) % NX) * CORES + c

    def sem_index(k1, k2):
        return k1 - 1 if k2 == 0 else {1: 3, 3: 7, 2: 11}[k2] + k1

    class Gather:
        def __init__(self, view, send_sem, recv_sems):
            self.view, self.send_sem, self.recv_sems = view, send_sem, recv_sems

        def push(self, k1, k2, dim, step, half=None):
            mine = ((k1 - step) % R, k2) if dim == 0 else (k1, (k2 - step) % R)
            ref = self.view(*place(*mine, c), half)
            remote(ref, ref, self.send_sem, self.recv_sems(sem_index(k1, k2)), *neighbour(dim, step)).start()

        def arrive(self, k1, k2):
            ref = self.view(*place(k1, k2, c), None)
            remote(ref, ref, self.send_sem, self.recv_sems(sem_index(k1, k2)), h, m).wait_recv()

        def own(self):
            self.push(2, 0, 0, 2)
            self.push(1, 0, 0, 1)
            self.push(3, 0, 0, -1)
            self.push(0, 1, 1, 1)
            self.push(0, 3, 1, -1)

        def stages(self, done=lambda k1, k2: None):
            def first(k1):
                self.arrive(k1, 0)
                self.push(k1, 1, 1, 1)
                self.push(k1, 3, 1, -1)
                done(k1, 0)

            def second(k1, k2):
                self.arrive(k1, k2)
                step = 2 - k2
                self.push(k1, 2, 1, step, half=(1 - step) // 2)
                done(k1, k2)

            def last(k1):
                self.arrive(k1, 2)
                done(k1, 2)

            order = [(first, 1), (first, 3), (second, 0, 1), (second, 0, 3), (first, 2), (second, 1, 1), (second, 1, 3), (second, 3, 1),
                     (second, 3, 3), (last, 0), (second, 2, 1), (second, 2, 3), (last, 1), (last, 3), (last, 2)]
            return [functools.partial(*stage) for stage in order]

    def o_view(g):
        def view(sy, sx, half):
            start, size = sy * qw, qw
            if half is not None:
                start, size = start + half * (qw // 2), qw // 2
            return o_v.at[sx, pl.ds(g * ROW_TILE, ROW_TILE), pl.ds(pl.multiple_of(start, size), size)]

        return view

    o_gathers = [
        Gather(o_view(g), a_ss, functools.partial(lambda g, idx: a_rs.at[g, idx], g)) for g in range(lr // ROW_TILE)
    ]

    def a_send_own(g):
        for j in range(qs):
            o_v[x, pl.ds(g * ROW_TILE, ROW_TILE), pl.ds(pl.multiple_of(h * qw + j * dh, dh), dh)] = (
                o_wide[pl.ds(g * ROW_TILE * qs + j, ROW_TILE, stride=qs), :].astype(BF16))
        o_gathers[g].own()

    groups = lr // ROW_TILE
    per_group = ROW_TILE // SEQ_STEP

    with jax.named_scope("first"):
        k_load(0).wait()
        scores_of(0)

    def body(i, carry):
        for g in range(groups - 1):
            @pl.when(i == (g + 1) * per_group + 1)
            def _():
                a_send_own(g)
        @pl.when(i == RELAY_STEP)
        def _():
            w_relay()

        @pl.when(i + AHEAD - 1 < steps)
        def _():
            kv_start(i + AHEAD - 1)

        k_load(i).wait()
        v_load(i - 1).wait()
        scores_of(i)
        values_of(i - 1)
        return carry

    with jax.named_scope("attn"):
        lax.fori_loop(1, steps, body, 0)
        v_load(steps - 1).wait()
        values_of(steps - 1)

    with jax.named_scope("a_own"):
        a_send_own(groups - 1)

    with jax.named_scope("w_wait"):
        own_load.wait()
        remote(blocks(R * R - 1), blocks(R * R - 1), w_sem.at[0], w_sem.at[1], h, m).wait_recv()
        remote(wo_v.at[:, c], wo_v.at[:, c], f_sem.at[0], f_sem.at[1], h, partner).start()

    with jax.named_scope("new_wait"):
        others = new_v.at[:, :, pl.ds(0, (H - 1) * kvw)]
        remote(others, others, n_sem.at[0], n_sem.at[1], h, m).wait_recv()
        for which in range(2):
            fresh_v[which] = new_v[which].astype(F32).reshape(fresh_v.shape[1:]).astype(BF16)

    o_stages = [gather.stages() for gather in o_gathers]
    for n, stage_group in enumerate(zip(*o_stages)):
        with jax.named_scope(f"a_stage#n={n}"):
            for stage in stage_group:
                stage()

    with jax.named_scope("f_wait"):
        remote(wo_v.at[:, 1 - c], wo_v.at[:, 1 - c], f_sem.at[0], f_sem.at[1], h, m).wait_recv()

    with jax.named_scope("proj"):
        mixed = jnp.dot(o_v[...].reshape(NX * lr, H * qw), wo_v[...].reshape(H * M * dh, cols), preferred_element_type=F32)
        mixed = tok_v[:, c, :, my_cols].astype(F32) + mixed.reshape(NX, lr, cols)
        out_v[:, c, :, my_cols] = mixed.astype(BF16)

    def out_view(core):
        def view(sy, sx, half):
            at = pl.ds(pl.multiple_of((sy * NX + sx) * cols, cols), cols)
            if half is None:
                return out_v.at[:, core, :, at]
            return out_v.at[pl.ds(half * (NX // 2), NX // 2), core, :, at]

        return view

    def d_copy(k1, k2, core):
        blk = out_view(core)(*place(k1, k2, core), None)
        return remote(blk, blk, d_sem.at[0], d_sem.at[1], h, partner)

    out_gather = Gather(out_view(c), g_ss, lambda idx: g_rs.at[idx])
    out_gather.own()
    d_copy(0, 0, c).start()
    for n, stage in enumerate(out_gather.stages(lambda k1, k2: d_copy(k1, k2, c).start())):
        with jax.named_scope(f"g_stage#n={n}"):
            stage()
    with jax.named_scope("d_wait"):
        remote(out_v.at[:, 1 - c], out_v.at[:, 1 - c], d_sem.at[0], d_sem.at[1], h, m).wait_recv()

    def sent(ref, sem):
        remote(ref, ref, sem, q_sem.at[1], h, m).wait_send()

    with jax.named_scope("s_wait"):
        sent(q_send.at[pl.ds(0, M - 1)], q_sem.at[0])
        sent(blocks(R * R - 1 + len(relays)), w_sem.at[0])
        sent(wo_v.at[:, c], f_sem.at[0])
        sent(new_v.at[:, :, pl.ds(0, (H - 1) * kvw)], n_sem.at[0])
        sent(blocks((R * R - 1) * (lr * qw) // (dh * cols)), a_ss)
        sent(blocks(R * R - 1), g_ss)
        sent(out_v.at[:, c], d_sem.at[0])


def store_kernel(out_v, fresh_v, out, key_out, value_out, sems):
    copies = [
        pltpu.make_async_copy(out_v, out, sems.at[0]),
        pltpu.make_async_copy(fresh_v.at[0], key_out, sems.at[1]),
        pltpu.make_async_copy(fresh_v.at[1], value_out, sems.at[2]),
    ]
    for cp in copies:
        cp.start()
    for cp in copies:
        cp.wait()


def solution(mesh):
    heads_count = mesh.shape["heads"]
    model_count = mesh.shape["model"]

    def local_step(tokens, w_query, w_key, w_value, w_out, key_cache, value_cache, lengths):
        batch_all, width = tokens.shape
        rows, kv_count, context, head_dim = key_cache.shape
        chips_x = model_count // CORES
        q_shard = model_count * (w_query.shape[1] // head_dim)
        group = q_shard * heads_count // kv_count
        kv_shard = q_shard // group
        cols = width // (heads_count * chips_x)
        dims = dict(heads=heads_count, chips_x=chips_x, rows=rows, context=context, head_dim=head_dim, width=width,
                    kv_shard=kv_shard, q_shard=q_shard, group=group, cols=cols, n_load=4)
        assert heads_count == chips_x == 4 and q_shard == model_count
        steps = rows // SEQ_STEP
        groups = rows // ROW_TILE
        ring = heads_count
        any_spec = pl.BlockSpec(memory_space=pl.ANY)
        dma = pltpu.SemaphoreType.DMA
        vmem_spec = pl.BlockSpec(memory_space=pltpu.VMEM)
        out_tok, fresh = pl.pallas_call(
            functools.partial(step_kernel, dims),
            out_shape=(
                pltpu.VMEM((chips_x, CORES, rows, width), BF16),
                pltpu.VMEM((2, rows, kv_count, head_dim), BF16),
            ),
            in_specs=[any_spec] * 7 + [pl.BlockSpec(memory_space=pltpu.SMEM)],
            out_specs=(vmem_spec,) * 2,
            scratch_shapes=[
                pltpu.VMEM((chips_x, CORES, rows, width), BF16),
                pltpu.VMEM((width, head_dim), BF16),
                pltpu.VMEM((2, width, kv_shard * head_dim), BF16),
                pltpu.VMEM((rows, kv_shard, context, head_dim), BF16),
                pltpu.VMEM((rows, kv_shard, context, head_dim), BF16),
                pltpu.VMEM((heads_count * chips_x, CORES, head_dim, cols), BF16),
                pltpu.VMEM((model_count, rows, head_dim), BF16),
                pltpu.VMEM((model_count, rows, head_dim), BF16),
                pltpu.VMEM((model_count * rows, head_dim), F32),
                pltpu.VMEM((2, rows, kv_count * head_dim), BF16),
                pltpu.VMEM((2 * kv_shard * rows, head_dim), F32),
                pltpu.VMEM((2, SEQ_STEP, q_shard, context), BF16),
                pltpu.VMEM((2, SEQ_STEP, q_shard, head_dim), F32),
                pltpu.VMEM((rows * q_shard, head_dim), F32),
                pltpu.VMEM((chips_x, rows, heads_count * q_shard * head_dim), BF16),
                pltpu.VMEM((7, head_dim, cols), BF16),
                dma((8,)),
                dma((2,)),
                dma((2, steps)),
                dma,
                dma((2,)),
                dma((2,)),
                dma,
                dma((2,)),
                dma((2,)),
                dma,
                dma((groups, ring * ring - 1)),
                dma,
                dma((ring * ring - 1,)),
                dma((2,)),
            ],
            compiler_params=pltpu.CompilerParams(
                collective_id=0, has_side_effects=True, vmem_limit_bytes=60 * 1024 * 1024
            ),
            name="decode_step",
        )(
            tokens.reshape(chips_x, CORES, rows, width), w_query, w_key, w_value, w_out, key_cache, value_cache, lengths
        )
        new_shape = jax.ShapeDtypeStruct((rows, kv_count, head_dim), BF16)
        out, key_new, value_new = pl.pallas_call(
            store_kernel,
            out_shape=(jax.ShapeDtypeStruct((chips_x, CORES, rows, width), BF16), new_shape, new_shape),
            in_specs=[any_spec] * 2,
            out_specs=(any_spec,) * 3,
            scratch_shapes=[dma((3,))],
            compiler_params=pltpu.CompilerParams(vmem_limit_bytes=1024 * 1024),
            name="store",
        )(out_tok, fresh)
        return out.reshape(batch_all, width), key_new, value_new

    cache_spec = P(("replica", "model"), None, None, None)
    new_spec = P(("replica", "model"), None, None)
    return jax.shard_map(
        local_step,
        mesh=mesh,
        in_specs=(P("replica", None), P(None, ("heads", "model")), P(None, None), P(None, None), P(("heads", "model"), None), cache_spec, cache_spec, P(("replica", "model"))),
        out_specs=(P("replica", None), new_spec, new_spec),
        check_vma=False,
    )
```
